32 devices in a mesh: px: 4 (over x, core), py: 2 (over y), pz: 4 (over z).
Axes of the slice: x: 2, y: 2, z: 4, core: 2. Of those that a mesh axis runs over, the one named last changes fastest.
Arguments:
- control_values: float32 [28, 14, 28, 512], P('px', 'py', 'pz'), may hold values from -6 to 6
- metric_diag: float32 [3, 32, 512], P(None, 'px', ('py', 'pz')), may hold values from 0.5 to 2
- metric_off: float32 [3, 32, 512], P(None, 'px', ('py', 'pz')), may hold values from -0.2 to 0.2
- mass_weight: float32 [32, 512], P('px', ('py', 'pz')), may hold values from 0.5 to 2
- orient: int32 [4, 2, 4, 3], P('px', 'py', 'pz'), may hold values from 0 to 1
Outputs:
- stiffness_out: float32 [28, 14, 28, 512], P('px', 'py', 'pz')
- mass_out: float32 [28, 14, 28, 512], P('px', 'py', 'pz')
The draws below stay inside these ranges and needn't reach their ends.
All inputs are finite; a program needn't handle non-finite values.
Results may differ from the reference program's by a relative error of at most 0.0003.
Values sent between devices are 32-bit elements; how exact they have to be, the bound alone decides.
A program may use at most 64 MiB of HBM per device.

```python
import math
import jax
import jax.numpy as jnp
import numpy as np
from jax import lax

ELEMS = 4
VECS = 512
CTRL = 7
QUAD = 8
N_PX = 4
N_PY = 2
N_PZ = 4


def touch_ends(drawn, own_key, smallest, top_value):
    shape = drawn.shape
    index_at = [jax.random.randint(jax.random.fold_in(own_key, axis), (), 0, shape[axis]) for axis in range(len(shape))]
    drawn = drawn.at[tuple(index_at)].set(smallest)
    longest = shape.index(max(shape))
    index_at[longest] = (index_at[longest] + 1) % shape[longest]
    return drawn.at[tuple(index_at)].set(top_value)


def levels(rng, dims, split, least, high):
    loudness = 1.0
    for axis_at, blocks in split:
        draws = jax.random.uniform(jax.random.fold_in(jax.random.fold_in(rng, 6), axis_at), (blocks,), jnp.float32, least / len(split), high / len(split))
        loudness = loudness * jnp.repeat(jnp.exp(draws), dims[axis_at] // blocks).reshape((-1,) + (1,) * (len(dims) - 1 - axis_at))
    return loudness


def bell_draw(stream_key, shape, deviation, most, split=(), held_as=jnp.bfloat16):
    result = deviation * jax.random.normal(stream_key, shape, jnp.float32)
    if split:
        result = result * levels(stream_key, shape, split, -0.22, 0.18)
    return jnp.clip(result, -most, most).astype(held_as)


def setup_inputs(seed: int = 0) -> dict:
    key_of = jax.random.split(jax.random.key(seed), 6)
    return {
        "control_values": bell_draw(key_of[0], (N_PX * CTRL, N_PY * CTRL, N_PZ * CTRL, VECS), 1.0, 6.0, ((0, 4), (1, 2), (2, 4)), jnp.float32),
        "metric_diag": jnp.clip(jnp.exp(math.log(2.0) - 1.3862944 * jax.random.uniform(key_of[1], (3, N_PX * QUAD, N_PY * N_PZ * QUAD * QUAD), jnp.float32) ** levels(key_of[1], (3, N_PX * QUAD, N_PY * N_PZ * QUAD * QUAD), ((1, 4), (2, 8)), -0.2, 0.2)), 0.5, 2.0),
        "metric_off": jnp.clip(jax.random.uniform(key_of[2], (3, N_PX * QUAD, N_PY * N_PZ * QUAD * QUAD), jnp.float32, -0.2, 0.2) * levels(key_of[2], (3, N_PX * QUAD, N_PY * N_PZ * QUAD * QUAD), ((1, 4), (2, 8)), -0.4, 0.0), -0.2, 0.2),
        "mass_weight": jnp.clip(jnp.exp(math.log(2.0) - 1.3862944 * jax.random.uniform(key_of[3], (N_PX * QUAD, N_PY * N_PZ * QUAD * QUAD), jnp.float32) ** levels(key_of[3], (N_PX * QUAD, N_PY * N_PZ * QUAD * QUAD), ((0, 4), (1, 8)), -0.2, 0.2)), 0.5, 2.0),
        "orient": touch_ends(jax.random.randint(key_of[4], (N_PX, N_PY, N_PZ, 3), 0, 2), jax.random.fold_in(key_of[4], 1), 0, 1).astype(jnp.int32),
    }


def spline_tables(elements):
    knot_row = np.concatenate([np.zeros(3), np.arange(elements + 1) * 1.0, np.full(3, float(elements))])
    offsets = np.array([0.5 - 0.5 / math.sqrt(3.0), 0.5 + 0.5 / math.sqrt(3.0)])
    points = (np.arange(elements)[:, None] + offsets[None, :]).reshape(-1)
    intervals = np.repeat(np.arange(elements), 2) + 3
    current = np.zeros((points.size, knot_row.size - 1))
    current[np.arange(points.size), intervals] = 1.0
    previous = current
    for degree in range(1, 4):
        columns = knot_row.size - 1 - degree
        updated = np.zeros((points.size, columns))
        for i in range(columns):
            lower_gap = knot_row[i + degree] - knot_row[i]
            upper_gap = knot_row[i + degree + 1] - knot_row[i + 1]
            if lower_gap > 0:
                updated[:, i] += (points - knot_row[i]) / lower_gap * current[:, i]
            if upper_gap > 0:
                updated[:, i] += (knot_row[i + degree + 1] - points) / upper_gap * current[:, i + 1]
        previous = current
        current = updated
    slopes = np.zeros(current.shape)
    for i in range(current.shape[1]):
        lower_gap = knot_row[i + 3] - knot_row[i]
        upper_gap = knot_row[i + 4] - knot_row[i + 1]
        if lower_gap > 0:
            slopes[:, i] += 3.0 / lower_gap * previous[:, i]
        if upper_gap > 0:
            slopes[:, i] -= 3.0 / upper_gap * previous[:, i + 1]
    return (current.astype(np.float32), slopes.astype(np.float32))

def contract(pattern, operand, table_part):
    return jnp.einsum(pattern, operand, table_part, precision=lax.Precision.HIGHEST)

def forward_parts(coeffs, values, slopes):
    along_b = contract('ijkv,ck->ijcv', coeffs, values)
    along_d = contract('ijkv,ck->ijcv', coeffs, slopes)
    plain = contract('ijcv,bj->ibcv', along_b, values)
    slope_y = contract('ijcv,bj->ibcv', along_b, slopes)
    slope_z = contract('ijcv,bj->ibcv', along_d, values)
    return (plain, slope_y, slope_z)

def stiffness_apply(parts, diag_terms, off_terms, values, slopes, block_rows):
    plain, slope_y, slope_z = parts
    quad_count = values.shape[0]
    back_x = jnp.zeros(plain.shape, jnp.float32)
    back_y = jnp.zeros(plain.shape, jnp.float32)
    back_z = jnp.zeros(plain.shape, jnp.float32)
    for first_row in range(0, quad_count, block_rows):
        last_row = first_row + block_rows
        slope_rows = slopes[first_row:last_row]
        value_rows = values[first_row:last_row]
        grad_x = contract('ibcv,ai->abcv', plain, slope_rows)
        grad_y = contract('ibcv,ai->abcv', slope_y, value_rows)
        grad_z = contract('ibcv,ai->abcv', slope_z, value_rows)
        diag_rows = diag_terms[:, first_row:last_row, :, :, None]
        off_rows = off_terms[:, first_row:last_row, :, :, None]
        flux_x = diag_rows[0] * grad_x + off_rows[0] * grad_y + off_rows[1] * grad_z
        flux_y = off_rows[0] * grad_x + diag_rows[1] * grad_y + off_rows[2] * grad_z
        flux_z = off_rows[1] * grad_x + off_rows[2] * grad_y + diag_rows[2] * grad_z
        back_x = back_x + contract('abcv,ai->ibcv', flux_x, slope_rows)
        back_y = back_y + contract('abcv,ai->ibcv', flux_y, value_rows)
        back_z = back_z + contract('abcv,ai->ibcv', flux_z, value_rows)
    middle_b = contract('ibcv,bj->ijcv', back_x, values) + contract('ibcv,bj->ijcv', back_y, slopes)
    middle_d = contract('ibcv,bj->ijcv', back_z, values)
    return contract('ijcv,ck->ijkv', middle_b, values) + contract('ijcv,ck->ijkv', middle_d, slopes)

def mass_apply(plain, weights, values, block_rows):
    quad_count = values.shape[0]
    back_mass = jnp.zeros(plain.shape, jnp.float32)
    for first_row in range(0, quad_count, block_rows):
        last_row = first_row + block_rows
        value_rows = values[first_row:last_row]
        point_values = contract('ibcv,ai->abcv', plain, value_rows)
        weighted = weights[first_row:last_row, :, :, None] * point_values
        back_mass = back_mass + contract('abcv,ai->ibcv', weighted, value_rows)
    middle = contract('ibcv,bj->ijcv', back_mass, values)
    return contract('ijcv,ck->ijkv', middle, values)

def flip_frame(grid_data, flip_flags, first_dim):
    for d in range(3):
        grid_data = jnp.where(flip_flags[d] == 1, jnp.flip(grid_data, axis=first_dim + d), grid_data)
    return grid_data

def fold_axis(grid_data, patch_axis, point_axis):
    extent = grid_data.shape[point_axis]
    first_plane = lax.slice_in_dim(grid_data, 0, 1, axis=point_axis)
    last_plane = lax.slice_in_dim(grid_data, extent - 1, extent, axis=point_axis)
    middle = lax.slice_in_dim(grid_data, 1, extent - 1, axis=point_axis)
    from_before = jnp.roll(last_plane, 1, axis=patch_axis)
    from_after = jnp.roll(first_plane, -1, axis=patch_axis)
    return jnp.concatenate([first_plane + from_before, middle, last_plane + from_after], axis=point_axis)

def reference(control_values, metric_diag, metric_off, mass_weight, orient):
    values_np, slopes_np = spline_tables(ELEMS)
    values = jnp.asarray(values_np)
    slopes = jnp.asarray(slopes_np)
    patches = N_PX * N_PY * N_PZ
    coeffs = control_values.reshape(N_PX, CTRL, N_PY, CTRL, N_PZ, CTRL, VECS)
    coeffs = coeffs.transpose(0, 2, 4, 1, 3, 5, 6).reshape(patches, CTRL, CTRL, CTRL, VECS)
    diag_all = metric_diag.reshape(3, N_PX, QUAD, N_PY, N_PZ, QUAD, QUAD)
    diag_all = diag_all.transpose(1, 3, 4, 0, 2, 5, 6).reshape(patches, 3, QUAD, QUAD, QUAD)
    off_all = metric_off.reshape(3, N_PX, QUAD, N_PY, N_PZ, QUAD, QUAD)
    off_all = off_all.transpose(1, 3, 4, 0, 2, 5, 6).reshape(patches, 3, QUAD, QUAD, QUAD)
    weight_all = mass_weight.reshape(N_PX, QUAD, N_PY, N_PZ, QUAD, QUAD)
    weight_all = weight_all.transpose(0, 2, 3, 1, 4, 5).reshape(patches, QUAD, QUAD, QUAD)
    flag_all = orient.reshape(patches, 3)

    def one_patch(patch_items):
        coeff_patch, diag_patch, off_patch, weight_patch, flag_patch = patch_items
        parts = forward_parts(coeff_patch, values, slopes)
        stiffness = stiffness_apply(parts, diag_patch, off_patch, values, slopes, QUAD)
        mass_part = mass_apply(parts[0], weight_patch, values, QUAD)
        return (flip_frame(stiffness, flag_patch, 0), flip_frame(mass_part, flag_patch, 0))
    stiffness_all, mass_all = lax.map(one_patch, (coeffs, diag_all, off_all, weight_all, flag_all))

    def assemble(grid_data):
        grid_data = grid_data.reshape(N_PX, N_PY, N_PZ, CTRL, CTRL, CTRL, VECS)
        grid_data = fold_axis(grid_data, 0, 3)
        grid_data = fold_axis(grid_data, 1, 4)
        grid_data = fold_axis(grid_data, 2, 5)
        return grid_data.reshape(patches, CTRL, CTRL, CTRL, VECS)

    def flip_back(patch_items):
        stiff_patch, mass_patch, flag_patch = patch_items
        return (flip_frame(stiff_patch, flag_patch, 0), flip_frame(mass_patch, flag_patch, 0))
    stiffness_all, mass_all = lax.map(flip_back, (assemble(stiffness_all), assemble(mass_all), flag_all))

    def to_layout(grid_data):
        grid_data = grid_data.reshape(N_PX, N_PY, N_PZ, CTRL, CTRL, CTRL, VECS)
        return grid_data.transpose(0, 3, 1, 4, 2, 5, 6).reshape(N_PX * CTRL, N_PY * CTRL, N_PZ * CTRL, VECS)
    return (to_layout(stiffness_all), to_layout(mass_all))
```

```python
import functools
import heapq
import math

import jax
import jax.numpy as jnp
import numpy as np
from jax import lax
from jax.experimental import pallas as pl
from jax.experimental.pallas import tpu as pltpu
from jax.sharding import PartitionSpec as P

LANES = 128
ROWS = 8
AXES = ("px", "py", "pz")


def spline_tables(elements):
    knot_row = np.concatenate(
        [np.zeros(3), np.arange(elements + 1) * 1.0, np.full(3, float(elements))]
    )
    offsets = np.array([0.5 - 0.5 / math.sqrt(3.0), 0.5 + 0.5 / math.sqrt(3.0)])
    points = (np.arange(elements)[:, None] + offsets[None, :]).reshape(-1)
    intervals = np.repeat(np.arange(elements), 2) + 3
    current = np.zeros((points.size, knot_row.size - 1))
    current[np.arange(points.size), intervals] = 1.0
    previous = current
    for degree in range(1, 4):
        columns = knot_row.size - 1 - degree
        updated = np.zeros((points.size, columns))
        for i in range(columns):
            lower_gap = knot_row[i + degree] - knot_row[i]
            upper_gap = knot_row[i + degree + 1] - knot_row[i + 1]
            if lower_gap > 0:
                updated[:, i] += (points - knot_row[i]) / lower_gap * current[:, i]
            if upper_gap > 0:
                updated[:, i] += (knot_row[i + degree + 1] - points) / upper_gap * current[:, i + 1]
        previous = current
        current = updated
    slopes = np.zeros(current.shape)
    for i in range(current.shape[1]):
        lower_gap = knot_row[i + 3] - knot_row[i]
        upper_gap = knot_row[i + 4] - knot_row[i + 1]
        if lower_gap > 0:
            slopes[:, i] += 3.0 / lower_gap * previous[:, i]
        if upper_gap > 0:
            slopes[:, i] -= 3.0 / upper_gap * previous[:, i + 1]
    return (current.astype(np.float32), slopes.astype(np.float32))


def split(x):
    high = x.astype(jnp.bfloat16)
    return high, (x - high.astype(jnp.float32)).astype(jnp.bfloat16)


def split_table(table):
    high = table.astype(jnp.bfloat16)
    low = (table - high.astype(np.float32)).astype(jnp.bfloat16)
    return np.asarray(high), np.asarray(low)


def plane_tables(values, slopes):
    quad, ctrl = values.shape
    wide = np.zeros((quad, ROWS), np.float64)
    tall = np.zeros((quad, ROWS), np.float64)
    wide[:, :ctrl] = values
    tall[:, :ctrl] = slopes
    fields = [np.kron(wide, wide), np.kron(tall, wide), np.kron(wide, tall)]
    forward = np.concatenate(fields, 0).astype(np.float32)
    high, low = split_table(forward)
    forward = np.concatenate([high, high, low], 1)
    backward = []
    size = ctrl * ROWS
    for flip_y in range(2):
        for flip_z in range(2):
            rows = np.full(size, -1)
            for j in range(ctrl):
                for k in range(ctrl):
                    jj = ctrl - 1 - j if flip_y else j
                    kk = ctrl - 1 - k if flip_z else k
                    rows[j * ROWS + k] = jj * ROWS + kk
            back = [np.where(rows[:, None] >= 0, f.T[rows], 0.0) for f in fields]
            none = np.zeros_like(back[0])
            stiff = np.concatenate([back[0], back[1], back[2], none], 1)
            mass = np.concatenate([none, none, none, back[0]], 1)
            high, low = split_table(np.concatenate([stiff, mass], 0).astype(np.float32))
            backward.append(np.concatenate([high, low], 0))
    return forward, np.stack(backward)


def apply_kernel(
    values, slopes, orient, u_ref, diag_ref, off_ref, weight_ref, fwd_ref, bwd_ref, out_ref,
    upad, square, coef, fields, back,
):
    quad, ctrl = values.shape
    width = u_ref.shape[3]
    points = quad * quad
    size = ctrl * ROWS

    @pl.when(pl.program_id(0) == 0)
    def _():
        upad[...] = jnp.zeros_like(upad)
        square[...] = jnp.zeros_like(square)
        for s in range(3):
            square[s * quad : (s + 1) * quad, 0:points] = diag_ref[s]
            square[(3 + s) * quad : (4 + s) * quad, 0:points] = off_ref[s]
        square[6 * quad : 7 * quad, 0:points] = weight_ref[...]
        turned = square[...].T
        for c in range(7 * quad):
            coef[c] = jnp.broadcast_to(turned[0:points, c : c + 1], (points, LANES))

    for i in range(ctrl):
        upad[i % 2, 0:ctrl, 0:ctrl, :] = u_ref[i]
        high, low = split(upad[i % 2].reshape(ROWS * ROWS, width))
        stacked = jnp.concatenate([high, low, high], axis=0)
        fields[i] = jnp.dot(fwd_ref[...], stacked, preferred_element_type=jnp.float32)

    @pl.loop(0, quad)
    def _(b):
        row = pl.multiple_of(b * ROWS, ROWS)
        for l in range(width // LANES):
            lanes = slice(l * LANES, (l + 1) * LANES)
            part = [
                [fields[i, pl.ds(f * points + row, ROWS), lanes] for f in range(3)]
                for i in range(ctrl)
            ]
            acc = [[None] * ctrl for _ in range(4)]
            for q in range(quad):
                near = [i for i in range(ctrl) if values[q, i] != 0.0 or slopes[q, i] != 0.0]
                v = {i: float(values[q, i]) for i in near}
                s = {i: float(slopes[q, i]) for i in near}
                g1 = sum(s[i] * part[i][0] for i in near)
                p = sum(v[i] * part[i][0] for i in near)
                g2 = sum(v[i] * part[i][1] for i in near)
                g3 = sum(v[i] * part[i][2] for i in near)
                d = [coef[t * quad + q, pl.ds(row, ROWS), :] for t in range(7)]
                flux = [
                    d[0] * g1 + d[3] * g2 + d[4] * g3,
                    d[3] * g1 + d[1] * g2 + d[5] * g3,
                    d[4] * g1 + d[5] * g2 + d[2] * g3,
                    d[6] * p,
                ]
                for f in range(4):
                    for i in near:
                        term = (s[i] if f == 0 else v[i]) * flux[f]
                        acc[f][i] = term if acc[f][i] is None else acc[f][i] + term
            for f in range(4):
                for i in range(ctrl):
                    back[i, pl.ds(f * points + row, ROWS), lanes] = acc[f][i]

    for i in range(ctrl):
        high, low = split(back[i])
        both = jnp.dot(bwd_ref[0], high, preferred_element_type=jnp.float32)
        rest = jnp.dot(bwd_ref[0, 0 : 2 * size], low, preferred_element_type=jnp.float32)
        total = both[0 : 2 * size] + both[2 * size : 4 * size] + rest
        to = jnp.where(orient[0] == 1, ctrl - 1 - i, i)
        for f in range(2):
            for l in range(width // LANES):
                out_ref[l, f, to] = total[f * size : (f + 1) * size, l * LANES : (l + 1) * LANES]


def apply_operator(u, diag, off, weight, orient, values, slopes):
    quad, ctrl = values.shape
    vecs = u.shape[3]
    width = 2 * LANES
    points = quad * quad
    size = ctrl * ROWS
    forward, backward = plane_tables(values, slopes)
    whole = lambda x: pl.BlockSpec(x.shape, lambda h, o: (0,) * x.ndim)
    grid_spec = pltpu.PrefetchScalarGridSpec(
        num_scalar_prefetch=1,
        grid=(vecs // width,),
        in_specs=[
            pl.BlockSpec((ctrl, ctrl, ctrl, width), lambda h, o: (0, 0, 0, h)),
            whole(diag),
            whole(off),
            whole(weight),
            whole(forward),
            pl.BlockSpec((1,) + backward.shape[1:], lambda h, o: (o[1] * 2 + o[2], 0, 0)),
        ],
        out_specs=pl.BlockSpec(
            (width // LANES, 2, ctrl, size, LANES), lambda h, o: (h, 0, 0, 0, 0)
        ),
        scratch_shapes=[
            pltpu.VMEM((2, ROWS, ROWS, width), jnp.float32),
            pltpu.VMEM((LANES, LANES), jnp.float32),
            pltpu.VMEM((7 * quad, points, LANES), jnp.float32),
            pltpu.VMEM((ctrl, 3 * points, width), jnp.float32),
            pltpu.VMEM((ctrl, 4 * points, width), jnp.float32),
        ],
    )
    return pl.pallas_call(
        functools.partial(apply_kernel, values, slopes),
        grid_spec=grid_spec,
        out_shape=jax.ShapeDtypeStruct((vecs // LANES, 2, ctrl, size, LANES), jnp.float32),
        name="apply_operator",
    )(orient, u, diag, off, weight, jnp.asarray(forward), jnp.asarray(backward))


ORDERS = ((1, 0, 2), (1, 2, 0), (0, 1, 2), (2, 0, 1))
WIRE = (1.07, 2.15, 1.07)
LATENCY = 1.8


def exchange_plan(chunks):
    free = [0.0, 0.0, 0.0]
    heap, plan = [], []

    def send(time, chunk, stage):
        d = ORDERS[chunk % 4][stage]
        free[d] = max(free[d], time) + WIRE[d]
        heapq.heappush(heap, (free[d] + LATENCY, chunk, stage))

    for chunk in range(chunks):
        send(0.0, chunk, 0)
    while heap:
        time, chunk, stage = heapq.heappop(heap)
        plan.append((chunk, stage))
        if stage < 2:
            send(time, chunk, stage + 1)
    return plan


def share_kernel(
    in_ref, out_ref, xbuf, ybuf, zbuf, zsend, send_sem, recv_sem,
):
    chunks, ctrl = in_ref.shape[0], in_ref.shape[2]
    nbrs = []
    for axis in AXES:
        size, me = lax.axis_size(axis), lax.axis_index(axis)
        nbrs.append((lax.rem(me + size - 1, size), lax.rem(me + 1, size)))
    barrier = pltpu.get_barrier_semaphore()
    for d in range(3):
        for side in range(2):
            pl.semaphore_signal(
                barrier,
                inc=1,
                device_id={AXES[d]: nbrs[d][side]},
                device_id_type=pl.DeviceIdType.MESH,
            )
    pl.semaphore_wait(barrier, 6)

    ends = (0, ctrl - 1)

    def copies(c, stage):
        d = ORDERS[c % 4][stage]
        src = in_ref if stage == 0 else out_ref
        result = []
        for side in range(2):
            e = ends[side]
            if d == 0:
                plane, buf = src.at[c, :, e], xbuf
            elif d == 1:
                plane, buf = src.at[c, :, :, e * ROWS : (e + 1) * ROWS], ybuf
            else:
                plane, buf = zsend.at[c, side], zbuf
            result.append(
                pltpu.make_async_remote_copy(
                    src_ref=plane,
                    dst_ref=buf.at[c, 1 - side],
                    send_sem=send_sem.at[c, d, side],
                    recv_sem=recv_sem.at[c, d, 1 - side],
                    device_id={AXES[d]: nbrs[d][side]},
                    device_id_type=pl.DeviceIdType.MESH,
                )
            )
        return result

    def start(c, stage):
        d = ORDERS[c % 4][stage]
        if d == 2:
            src = in_ref if stage == 0 else out_ref
            for side in range(2):
                for f in range(2):
                    for i in range(ctrl):
                        zsend[c, side, f, i] = src[
                            c, f, i, pl.ds(ends[side], ctrl, stride=ROWS), :
                        ]
        for copy in copies(c, stage):
            copy.start()

    for c in range(chunks):
        start(c, 0)
    out_ref[...] = in_ref[...]
    for c, stage in exchange_plan(chunks):
        d = ORDERS[c % 4][stage]
        for copy in copies(c, stage):
            copy.wait()
        for side in range(2):
            e = ends[side]
            for f in range(2):
                if d == 0:
                    out_ref[c, f, e] += xbuf[c, side, f]
                elif d == 1:
                    for i in range(ctrl):
                        out_ref[c, f, i, e * ROWS : (e + 1) * ROWS] += ybuf[c, side, f, i]
                else:
                    for i in range(ctrl):
                        rows = pl.ds(e, ctrl, stride=ROWS)
                        out_ref[c, f, i, rows, :] = (
                            out_ref[c, f, i, rows, :] + zbuf[c, side, f, i]
                        )
        if stage < 2:
            start(c, stage + 1)


def share_points(parts):
    chunks, _, ctrl, size, lanes = parts.shape
    return pl.pallas_call(
        share_kernel,
        out_shape=jax.ShapeDtypeStruct(parts.shape, parts.dtype),
        in_specs=[pl.BlockSpec(memory_space=pltpu.VMEM)],
        out_specs=pl.BlockSpec(memory_space=pltpu.VMEM),
        scratch_shapes=[
            pltpu.VMEM((chunks, 2, 2, size, lanes), jnp.float32),
            pltpu.VMEM((chunks, 2, 2, ctrl, ROWS, lanes), jnp.float32),
            pltpu.VMEM((chunks, 2, 2, ctrl, ctrl, lanes), jnp.float32),
            pltpu.VMEM((chunks, 2, 2, ctrl, ctrl, lanes), jnp.float32),
            pltpu.SemaphoreType.DMA((chunks, 3, 2)),
            pltpu.SemaphoreType.DMA((chunks, 3, 2)),
        ],
        compiler_params=pltpu.CompilerParams(collective_id=0, has_side_effects=True),
        name="share_points",
    )(parts)


def turn_kernel(orient, in_ref, stiff_ref, mass_ref):
    ctrl = in_ref.shape[2]
    lanes = in_ref.shape[4]

    def turn(reverse):
        index = ctrl - 1 - lax.broadcasted_iota(jnp.int32, (ROWS, lanes), 0)
        index = jnp.maximum(index, 0)
        for f, ref in enumerate((stiff_ref, mass_ref)):
            for i in range(ctrl):
                from_i = jnp.where(orient[0] == 1, ctrl - 1 - i, i)
                for j in range(ctrl):
                    from_j = jnp.where(orient[1] == 1, ctrl - 1 - j, j)
                    row = pl.multiple_of(from_j * ROWS, ROWS)
                    x = in_ref[0, f, from_i, pl.ds(row, ROWS), :]
                    if reverse:
                        x = jnp.take_along_axis(x, index, axis=0, mode="promise_in_bounds")
                    ref[i, j] = x[0:ctrl]

    @pl.when(orient[2] == 1)
    def _():
        turn(True)

    @pl.when(orient[2] != 1)
    def _():
        turn(False)


def turn_back(shared, orient):
    chunks, _, ctrl, size, lanes = shared.shape
    shape = (ctrl, ctrl, ctrl, chunks * lanes)
    out = pl.BlockSpec((ctrl, ctrl, ctrl, lanes), lambda c, o: (0, 0, 0, c))
    return pl.pallas_call(
        turn_kernel,
        grid_spec=pltpu.PrefetchScalarGridSpec(
            num_scalar_prefetch=1,
            grid=(chunks,),
            in_specs=[
                pl.BlockSpec((1, 2, ctrl, size, lanes), lambda c, o: (c, 0, 0, 0, 0))
            ],
            out_specs=[out, out],
        ),
        out_shape=[jax.ShapeDtypeStruct(shape, jnp.float32)] * 2,
        name="turn_back",
    )(orient, shared)


def per_device(control_values, metric_diag, metric_off, mass_weight, orient):
    values, slopes = spline_tables(mass_weight.shape[0] // 2)
    flags = orient.reshape(3)
    parts = apply_operator(
        control_values, metric_diag, metric_off, mass_weight, flags, values, slopes
    )
    return tuple(turn_back(share_points(parts), flags))


def solution(mesh):
    in_specs = (
        P("px", "py", "pz", None),
        P(None, "px", ("py", "pz")),
        P(None, "px", ("py", "pz")),
        P("px", ("py", "pz")),
        P("px", "py", "pz", None),
    )
    out_specs = (P("px", "py", "pz", None), P("px", "py", "pz", None))
    return jax.shard_map(
        per_device, mesh=mesh, in_specs=in_specs, out_specs=out_specs, check_vma=False
    )
```

```python
import functools
import heapq
import math

import jax
import jax.numpy as jnp
import numpy as np
from jax import lax
from jax.experimental import pallas as pl
from jax.experimental.pallas import tpu as pltpu
from jax.sharding import PartitionSpec as P

LANES = 128
ROWS = 8
AXES = ("px", "py", "pz")


def spline_tables(elements):
    knot_row = np.concatenate(
        [np.zeros(3), np.arange(elements + 1) * 1.0, np.full(3, float(elements))]
    )
    offsets = np.array([0.5 - 0.5 / math.sqrt(3.0), 0.5 + 0.5 / math.sqrt(3.0)])
    points = (np.arange(elements)[:, None] + offsets[None, :]).reshape(-1)
    intervals = np.repeat(np.arange(elements), 2) + 3
    current = np.zeros((points.size, knot_row.size - 1))
    current[np.arange(points.size), intervals] = 1.0
    previous = current
    for degree in range(1, 4):
        columns = knot_row.size - 1 - degree
        updated = np.zeros((points.size, columns))
        for i in range(columns):
            lower_gap = knot_row[i + degree] - knot_row[i]
            upper_gap = knot_row[i + degree + 1] - knot_row[i + 1]
            if lower_gap > 0:
                updated[:, i] += (points - knot_row[i]) / lower_gap * current[:, i]
            if upper_gap > 0:
                updated[:, i] += (knot_row[i + degree + 1] - points) / upper_gap * current[:, i + 1]
        previous = current
        current = updated
    slopes = np.zeros(current.shape)
    for i in range(current.shape[1]):
        lower_gap = knot_row[i + 3] - knot_row[i]
        upper_gap = knot_row[i + 4] - knot_row[i + 1]
        if lower_gap > 0:
            slopes[:, i] += 3.0 / lower_gap * previous[:, i]
        if upper_gap > 0:
            slopes[:, i] -= 3.0 / upper_gap * previous[:, i + 1]
    return (current.astype(np.float32), slopes.astype(np.float32))


def split(x):
    high = x.astype(jnp.bfloat16)
    return high, (x - high.astype(jnp.float32)).astype(jnp.bfloat16)


def split_table(table):
    high = table.astype(jnp.bfloat16)
    low = (table - high.astype(np.float32)).astype(jnp.bfloat16)
    return np.asarray(high), np.asarray(low)


def plane_tables(values, slopes):
    quad, ctrl = values.shape
    wide = np.zeros((quad, ROWS), np.float64)
    tall = np.zeros((quad, ROWS), np.float64)
    wide[:, :ctrl] = values
    tall[:, :ctrl] = slopes
    fields = [np.kron(wide, wide), np.kron(tall, wide), np.kron(wide, tall)]
    forward = np.concatenate(fields, 0).astype(np.float32)
    high, low = split_table(forward)
    forward = np.concatenate([high, high, low], 1)
    backward = []
    size = ctrl * ROWS
    for flip_y in range(2):
        for flip_z in range(2):
            rows = np.full(size, -1)
            for j in range(ctrl):
                for k in range(ctrl):
                    jj = ctrl - 1 - j if flip_y else j
                    kk = ctrl - 1 - k if flip_z else k
                    rows[j * ROWS + k] = jj * ROWS + kk
            back = [np.where(rows[:, None] >= 0, f.T[rows], 0.0) for f in fields]
            none = np.zeros_like(back[0])
            stiff = np.concatenate([back[0], back[1], back[2], none], 1)
            mass = np.concatenate([none, none, none, back[0]], 1)
            backward.append(np.concatenate([stiff, mass], 0).astype(np.float32))
    return forward, np.stack(backward)


def make_copies(orders, zsend, bufs, state, send_sem, recv_sem, nbrs, c, stage):
    ctrl = state.shape[2]
    d = orders[c % len(orders)][stage]
    result = []
    for side in range(2):
        e = side * (ctrl - 1)
        if d == 0:
            plane = state.at[c, :, e]
        elif d == 1:
            plane = state.at[c, :, :, e * ROWS : e * ROWS + ctrl]
        else:
            plane = zsend.at[c, side]
        result.append(
            pltpu.make_async_remote_copy(
                src_ref=plane,
                dst_ref=bufs[d].at[c, 1 - side],
                send_sem=send_sem.at[c, d, side],
                recv_sem=recv_sem.at[c, d, 1 - side],
                device_id={AXES[d]: nbrs[d][side]},
                device_id_type=pl.DeviceIdType.MESH,
            )
        )
    return result


def patch_kernel(
    values, slopes, orient, u_hbm, diag_ref, off_ref, weight_ref, fwd_ref, bwd_ref,
    stiff_hbm, mass_hbm,
    ubuf, upad, square, coef, fields, back, table, state, xbuf, ybuf, zbuf, zsend, turned,
    u_sem, out_sem, send_sem, recv_sem,
):
    quad, ctrl = values.shape
    vecs = u_hbm.shape[3]
    halves, width = ubuf.shape[0], ubuf.shape[4]
    chunks = vecs // LANES
    per_half = width // LANES
    points = quad * quad
    size = ctrl * ROWS
    bufs = (xbuf, ybuf, zbuf)

    loads = [
        pltpu.make_async_copy(
            u_hbm.at[:, :, :, h * width : (h + 1) * width], ubuf.at[h], u_sem.at[h]
        )
        for h in range(halves)
    ]
    for load in loads:
        load.start()

    nbrs = []
    for axis in AXES:
        count, me = lax.axis_size(axis), lax.axis_index(axis)
        nbrs.append((lax.rem(me + count - 1, count), lax.rem(me + 1, count)))
    barrier = pltpu.get_barrier_semaphore()
    for d in range(3):
        for side in range(2):
            pl.semaphore_signal(
                barrier,
                inc=1,
                device_id={AXES[d]: nbrs[d][side]},
                device_id_type=pl.DeviceIdType.MESH,
            )

    upad[...] = jnp.zeros_like(upad)
    square[...] = jnp.zeros_like(square)
    for s in range(3):
        square[s * quad : (s + 1) * quad, 0:points] = diag_ref[s]
        square[(3 + s) * quad : (4 + s) * quad, 0:points] = off_ref[s]
    square[6 * quad : 7 * quad, 0:points] = weight_ref[...]
    across = square[...].T
    for c in range(7 * quad):
        coef[c] = jnp.broadcast_to(across[0:points, c : c + 1], (points, LANES))

    def flips(shape):
        return [jnp.full(shape, orient[d], jnp.int32) == 1 for d in range(3)]

    _, flip_y, flip_z = flips(bwd_ref.shape[1:])
    high, low = split(
        jnp.where(
            flip_y,
            jnp.where(flip_z, bwd_ref[3], bwd_ref[2]),
            jnp.where(flip_z, bwd_ref[1], bwd_ref[0]),
        )
    )
    table[0 : 2 * size] = high
    table[2 * size : 4 * size] = low

    def operate(h):
        for i in range(ctrl):
            upad[i % 2, 0:ctrl, 0:ctrl, :] = ubuf[h, i]
            high, low = split(upad[i % 2].reshape(ROWS * ROWS, width))
            stacked = jnp.concatenate([high, low, high], axis=0)
            fields[i] = jnp.dot(fwd_ref[...], stacked, preferred_element_type=jnp.float32)

        @pl.loop(0, quad)
        def _(b):
            row = pl.multiple_of(b * ROWS, ROWS)
            for l in range(per_half):
                lanes = slice(l * LANES, (l + 1) * LANES)
                part = [
                    [fields[i, pl.ds(f * points + row, ROWS), lanes] for f in range(3)]
                    for i in range(ctrl)
                ]
                acc = [[None] * ctrl for _ in range(4)]
                for q in range(quad):
                    near = [i for i in range(ctrl) if values[q, i] != 0.0 or slopes[q, i] != 0.0]
                    v = {i: float(values[q, i]) for i in near}
                    s = {i: float(slopes[q, i]) for i in near}
                    g1 = sum(s[i] * part[i][0] for i in near)
                    p = sum(v[i] * part[i][0] for i in near)
                    g2 = sum(v[i] * part[i][1] for i in near)
                    g3 = sum(v[i] * part[i][2] for i in near)
                    d = [coef[t * quad + q, pl.ds(row, ROWS), :] for t in range(7)]
                    flux = [
                        d[0] * g1 + d[3] * g2 + d[4] * g3,
                        d[3] * g1 + d[1] * g2 + d[5] * g3,
                        d[4] * g1 + d[5] * g2 + d[2] * g3,
                        d[6] * p,
                    ]
                    for f in range(4):
                        for i in near:
                            term = (s[i] if f == 0 else v[i]) * flux[f]
                            acc[f][i] = term if acc[f][i] is None else acc[f][i] + term
                for f in range(4):
                    for i in range(ctrl):
                        back[i, pl.ds(f * points + row, ROWS), lanes] = acc[f][i]

        flip = flips((4 * points, width))[0]
        for i in range(ctrl):
            high, low = split(jnp.where(flip, back[ctrl - 1 - i], back[i]))
            both = jnp.dot(table[...], high, preferred_element_type=jnp.float32)
            rest = jnp.dot(table[0 : 2 * size], low, preferred_element_type=jnp.float32)
            total = both[0 : 2 * size] + both[2 * size : 4 * size] + rest
            for f in range(2):
                for l in range(per_half):
                    lanes = slice(l * LANES, (l + 1) * LANES)
                    state[h * per_half + l, f, i] = total[f * size : (f + 1) * size, lanes]

    copies = functools.partial(
        make_copies, ORDERS, zsend, bufs, state, send_sem, recv_sem, nbrs
    )

    def start(c, stage):
        if ORDERS[c % len(ORDERS)][stage] == 2:
            for side in range(2):
                for f in range(2):
                    for i in range(ctrl):
                        rows = pl.ds(side * (ctrl - 1), ctrl, stride=ROWS)
                        zsend[c, side, f, i] = state[c, f, i, rows, :]
        for copy in copies(c, stage):
            copy.start()

    for h in range(halves):
        loads[h].wait()
        operate(h)
        if h == 0:
            pl.semaphore_wait(barrier, 6)
        for l in range(per_half):
            start(h * per_half + l, 0)

    index = lax.broadcasted_iota(jnp.int32, (ROWS, LANES), 0)
    index = jnp.maximum(ctrl - 1 - index, 0)
    flip_x, flip_y, flip_z = flips((ROWS, LANES))
    stores = []
    for c, stage in exchange_plan(chunks, per_half):
        d = ORDERS[c % len(ORDERS)][stage]
        for copy in copies(c, stage):
            copy.wait()
        for side in range(2):
            e = side * (ctrl - 1)
            for f in range(2):
                if d == 0:
                    state[c, f, e] += xbuf[c, side, f]
                    continue
                for i in range(ctrl):
                    if d == 1:
                        state[c, f, i, e * ROWS : e * ROWS + ctrl] += ybuf[c, side, f, i]
                    else:
                        rows = pl.ds(e, ctrl, stride=ROWS)
                        state[c, f, i, rows, :] = state[c, f, i, rows, :] + zbuf[c, side, f, i]
        if stage < 2:
            start(c, stage + 1)
            continue
        lanes = slice(c * LANES, (c + 1) * LANES)
        for f in range(2):
            for i in range(ctrl):
                for j in range(ctrl):
                    x = [
                        [state[c, f, ii, jj * ROWS : (jj + 1) * ROWS] for jj in (j, ctrl - 1 - j)]
                        for ii in (i, ctrl - 1 - i)
                    ]
                    x = [jnp.where(flip_y, y[1], y[0]) for y in x]
                    x = jnp.where(flip_x, x[1], x[0])
                    other = jnp.take_along_axis(x, index, axis=0, mode="promise_in_bounds")
                    turned[f, i, j, :, lanes] = jnp.where(flip_z, other, x)[0:ctrl]
            store = pltpu.make_async_copy(
                turned.at[f, :, :, :, lanes],
                (stiff_hbm, mass_hbm)[f].at[:, :, :, lanes],
                out_sem.at[c, f],
            )
            store.start()
            stores.append(store)
    for store in stores:
        store.wait()


ORDERS = ((0, 1, 2), (0, 1, 2), (0, 2, 1), (2, 1, 0))
WIRE = (1.23, 2.15, 2.15)
LATENCY = (2.2, 2.2, 3.4)


def exchange_plan(chunks, per_half):
    free = [0.0, 0.0, 0.0]
    heap, plan = [], []

    def send(time, chunk, stage):
        d = ORDERS[chunk % len(ORDERS)][stage]
        free[d] = max(free[d], time) + WIRE[d]
        heapq.heappush(heap, (free[d] + LATENCY[d], chunk, stage))

    for chunk in range(chunks):
        send(3.0 * (chunk // per_half), chunk, 0)
    now = 0.0
    while heap:
        time, chunk, stage = heapq.heappop(heap)
        now = max(now, time) + 0.3
        plan.append((chunk, stage))
        if stage < 2:
            send(now, chunk, stage + 1)
    return plan


def apply_patch(u, diag, off, weight, orient, values, slopes):
    quad, ctrl = values.shape
    vecs = u.shape[3]
    width = 2 * LANES
    halves = vecs // width
    chunks = vecs // LANES
    points = quad * quad
    size = ctrl * ROWS
    forward, backward = plane_tables(values, slopes)
    vmem = pl.BlockSpec(memory_space=pltpu.VMEM)
    hbm = pl.BlockSpec(memory_space=pl.ANY)
    f32 = jnp.float32
    return pl.pallas_call(
        functools.partial(patch_kernel, values, slopes),
        out_shape=[jax.ShapeDtypeStruct(u.shape, f32)] * 2,
        in_specs=[pl.BlockSpec(memory_space=pltpu.SMEM), hbm] + [vmem] * 5,
        out_specs=[hbm, hbm],
        scratch_shapes=[
            pltpu.VMEM((halves, ctrl, ctrl, ctrl, width), f32),
            pltpu.VMEM((2, ROWS, ROWS, width), f32),
            pltpu.VMEM((LANES, LANES), f32),
            pltpu.VMEM((7 * quad, points, LANES), f32),
            pltpu.VMEM((ctrl, 3 * points, width), f32),
            pltpu.VMEM((ctrl, 4 * points, width), f32),
            pltpu.VMEM((4 * size, 4 * points), jnp.bfloat16),
            pltpu.VMEM((chunks, 2, ctrl, size, LANES), f32),
            pltpu.VMEM((chunks, 2, 2, size, LANES), f32),
            pltpu.VMEM((chunks, 2, 2, ctrl, ctrl, LANES), f32),
            pltpu.VMEM((chunks, 2, 2, ctrl, ctrl, LANES), f32),
            pltpu.VMEM((chunks, 2, 2, ctrl, ctrl, LANES), f32),
            pltpu.VMEM((2, ctrl, ctrl, ctrl, vecs), f32),
            pltpu.SemaphoreType.DMA((halves,)),
            pltpu.SemaphoreType.DMA((chunks, 2)),
            pltpu.SemaphoreType.DMA((chunks, 3, 2)),
            pltpu.SemaphoreType.DMA((chunks, 3, 2)),
        ],
        compiler_params=pltpu.CompilerParams(collective_id=0, has_side_effects=True),
        name="apply_patch",
    )(orient, u, diag, off, weight, jnp.asarray(forward), jnp.asarray(backward))


def per_device(control_values, metric_diag, metric_off, mass_weight, orient):
    values, slopes = spline_tables(mass_weight.shape[0] // 2)
    return tuple(
        apply_patch(
            control_values, metric_diag, metric_off, mass_weight, orient.reshape(3), values, slopes
        )
    )


def solution(mesh):
    in_specs = (
        P("px", "py", "pz", None),
        P(None, "px", ("py", "pz")),
        P(None, "px", ("py", "pz")),
        P("px", ("py", "pz")),
        P("px", "py", "pz", None),
    )
    out_specs = (P("px", "py", "pz", None), P("px", "py", "pz", None))
    return jax.shard_map(
        per_device, mesh=mesh, in_specs=in_specs, out_specs=out_specs, check_vma=False
    )
```

```python
import functools
import heapq
import math

import jax
import jax.numpy as jnp
import numpy as np
from jax import lax
from jax.experimental import pallas as pl
from jax.experimental.pallas import tpu as pltpu
from jax.sharding import PartitionSpec as P

LANES = 128
ROWS = 8
AXES = ("px", "py", "pz")


def spline_tables(elements):
    knot_row = np.concatenate(
        [np.zeros(3), np.arange(elements + 1) * 1.0, np.full(3, float(elements))]
    )
    offsets = np.array([0.5 - 0.5 / math.sqrt(3.0), 0.5 + 0.5 / math.sqrt(3.0)])
    points = (np.arange(elements)[:, None] + offsets[None, :]).reshape(-1)
    intervals = np.repeat(np.arange(elements), 2) + 3
    current = np.zeros((points.size, knot_row.size - 1))
    current[np.arange(points.size), intervals] = 1.0
    previous = current
    for degree in range(1, 4):
        columns = knot_row.size - 1 - degree
        updated = np.zeros((points.size, columns))
        for i in range(columns):
            lower_gap = knot_row[i + degree] - knot_row[i]
            upper_gap = knot_row[i + degree + 1] - knot_row[i + 1]
            if lower_gap > 0:
                updated[:, i] += (points - knot_row[i]) / lower_gap * current[:, i]
            if upper_gap > 0:
                updated[:, i] += (knot_row[i + degree + 1] - points) / upper_gap * current[:, i + 1]
        previous = current
        current = updated
    slopes = np.zeros(current.shape)
    for i in range(current.shape[1]):
        lower_gap = knot_row[i + 3] - knot_row[i]
        upper_gap = knot_row[i + 4] - knot_row[i + 1]
        if lower_gap > 0:
            slopes[:, i] += 3.0 / lower_gap * previous[:, i]
        if upper_gap > 0:
            slopes[:, i] -= 3.0 / upper_gap * previous[:, i + 1]
    return (current.astype(np.float32), slopes.astype(np.float32))


def split(x):
    high = x.astype(jnp.bfloat16)
    return high, (x - high.astype(jnp.float32)).astype(jnp.bfloat16)


def split_table(table):
    high = table.astype(jnp.bfloat16)
    low = (table - high.astype(np.float32)).astype(jnp.bfloat16)
    return np.asarray(high), np.asarray(low)


def plane_tables(values, slopes):
    quad, ctrl = values.shape
    wide = np.zeros((quad, ROWS), np.float64)
    tall = np.zeros((quad, ROWS), np.float64)
    wide[:, :ctrl] = values
    tall[:, :ctrl] = slopes
    fields = [np.kron(wide, wide), np.kron(tall, wide), np.kron(wide, tall)]
    forward = np.concatenate(fields, 0).astype(np.float32)
    high, low = split_table(forward)
    forward = np.concatenate([high, high, low], 1)
    backward = []
    size = ctrl * ROWS
    for flip_y in range(2):
        for flip_z in range(2):
            rows = np.full(size, -1)
            for j in range(ctrl):
                for k in range(ctrl):
                    jj = ctrl - 1 - j if flip_y else j
                    kk = ctrl - 1 - k if flip_z else k
                    rows[j * ROWS + k] = jj * ROWS + kk
            back = [np.where(rows[:, None] >= 0, f.T[rows], 0.0) for f in fields]
            none = np.zeros_like(back[0])
            stiff = np.concatenate([back[0], back[1], back[2], none], 1)
            mass = np.concatenate([none, none, none, back[0]], 1)
            backward.append(np.concatenate([stiff, mass], 0).astype(np.float32))
    return forward, np.stack(backward)


def make_copies(orders, zsend, bufs, state, send_sem, recv_sem, nbrs, c, stage):
    ctrl = state.shape[2]
    d = orders[c % len(orders)][stage]
    result = []
    for side in range(2):
        e = side * (ctrl - 1)
        if d == 0:
            plane = state.at[c, :, e]
        elif d == 1:
            plane = state.at[c, :, :, e * ROWS : e * ROWS + ctrl]
        else:
            plane = zsend.at[c, side]
        result.append(
            pltpu.make_async_remote_copy(
                src_ref=plane,
                dst_ref=bufs[d].at[c, 1 - side],
                send_sem=send_sem.at[c, d, side],
                recv_sem=recv_sem.at[c, d, 1 - side],
                device_id={AXES[d]: nbrs[d][side]},
                device_id_type=pl.DeviceIdType.MESH,
            )
        )
    return result


def patch_kernel(
    values, slopes, orient, u_hbm, diag_ref, off_ref, weight_ref, fwd_ref, bwd_ref,
    stiff_hbm, mass_hbm,
    ubuf, upad, square, coef, fields, back, table, state, xbuf, ybuf, zbuf, zsend, turned,
    u_sem, out_sem, send_sem, recv_sem,
):
    quad, ctrl = values.shape
    vecs = u_hbm.shape[3]
    halves, width = ubuf.shape[0], ubuf.shape[4]
    chunks = vecs // LANES
    per_half = width // LANES
    points = quad * quad
    size = ctrl * ROWS
    bufs = (xbuf, ybuf, zbuf)

    loads = [
        pltpu.make_async_copy(
            u_hbm.at[:, :, :, h * width : (h + 1) * width], ubuf.at[h], u_sem.at[h]
        )
        for h in range(halves)
    ]
    for load in loads:
        load.start()

    nbrs = []
    for axis in AXES:
        count, me = lax.axis_size(axis), lax.axis_index(axis)
        nbrs.append((lax.rem(me + count - 1, count), lax.rem(me + 1, count)))
    barrier = pltpu.get_barrier_semaphore()
    for d in range(3):
        for side in range(2):
            pl.semaphore_signal(
                barrier,
                inc=1,
                device_id={AXES[d]: nbrs[d][side]},
                device_id_type=pl.DeviceIdType.MESH,
            )

    upad[...] = jnp.zeros_like(upad)
    square[...] = jnp.zeros_like(square)
    for s in range(3):
        square[s * quad : (s + 1) * quad, 0:points] = diag_ref[s]
        square[(3 + s) * quad : (4 + s) * quad, 0:points] = off_ref[s]
    square[6 * quad : 7 * quad, 0:points] = weight_ref[...]
    across = square[...].T
    for c in range(7 * quad):
        coef[c] = jnp.broadcast_to(across[0:points, c : c + 1], (points, LANES))

    def flips(shape):
        return [jnp.full(shape, orient[d], jnp.int32) == 1 for d in range(3)]

    _, flip_y, flip_z = flips(bwd_ref.shape[1:])
    high, low = split(
        jnp.where(
            flip_y,
            jnp.where(flip_z, bwd_ref[3], bwd_ref[2]),
            jnp.where(flip_z, bwd_ref[1], bwd_ref[0]),
        )
    )
    table[0 : 2 * size] = high
    table[2 * size : 4 * size] = low

    def operate(h):
        for i in range(ctrl):
            upad[i % 2, 0:ctrl, 0:ctrl, :] = ubuf[h, i]
            high, low = split(upad[i % 2].reshape(ROWS * ROWS, width))
            stacked = jnp.concatenate([high, low, high], axis=0)
            fields[i] = jnp.dot(fwd_ref[...], stacked, preferred_element_type=jnp.float32)

        @pl.loop(0, quad)
        def _(b):
            row = pl.multiple_of(b * ROWS, ROWS)
            for l in range(per_half):
                lanes = slice(l * LANES, (l + 1) * LANES)
                part = [
                    [fields[i, pl.ds(f * points + row, ROWS), lanes] for f in range(3)]
                    for i in range(ctrl)
                ]
                acc = [[None] * ctrl for _ in range(4)]
                for q in range(quad):
                    near = [i for i in range(ctrl) if values[q, i] != 0.0 or slopes[q, i] != 0.0]
                    v = {i: float(values[q, i]) for i in near}
                    s = {i: float(slopes[q, i]) for i in near}
                    g1 = sum(s[i] * part[i][0] for i in near)
                    p = sum(v[i] * part[i][0] for i in near)
                    g2 = sum(v[i] * part[i][1] for i in near)
                    g3 = sum(v[i] * part[i][2] for i in near)
                    d = [coef[t * quad + q, pl.ds(row, ROWS), :] for t in range(7)]
                    flux = [
                        d[0] * g1 + d[3] * g2 + d[4] * g3,
                        d[3] * g1 + d[1] * g2 + d[5] * g3,
                        d[4] * g1 + d[5] * g2 + d[2] * g3,
                        d[6] * p,
                    ]
                    for f in range(4):
                        for i in near:
                            term = (s[i] if f == 0 else v[i]) * flux[f]
                            acc[f][i] = term if acc[f][i] is None else acc[f][i] + term
                for f in range(4):
                    for i in range(ctrl):
                        back[i, pl.ds(f * points + row, ROWS), lanes] = acc[f][i]

        flip = flips((4 * points, width))[0]
        for i in range(ctrl):
            high, low = split(jnp.where(flip, back[ctrl - 1 - i], back[i]))
            both = jnp.dot(table[...], high, preferred_element_type=jnp.float32)
            rest = jnp.dot(table[0 : 2 * size], low, preferred_element_type=jnp.float32)
            total = both[0 : 2 * size] + both[2 * size : 4 * size] + rest
            for f in range(2):
                for l in range(per_half):
                    lanes = slice(l * LANES, (l + 1) * LANES)
                    state[h * per_half + l, f, i] = total[f * size : (f + 1) * size, lanes]

    copies = functools.partial(
        make_copies, ORDERS, zsend, bufs, state, send_sem, recv_sem, nbrs
    )

    def start(c, stage):
        if ORDERS[c % len(ORDERS)][stage] == 2:
            for side in range(2):
                for f in range(2):
                    for i in range(ctrl):
                        rows = pl.ds(side * (ctrl - 1), ctrl, stride=ROWS)
                        zsend[c, side, f, i] = state[c, f, i, rows, :]
        for copy in copies(c, stage):
            copy.start()

    index = lax.broadcasted_iota(jnp.int32, (ROWS, LANES), 0)
    index = jnp.maximum(ctrl - 1 - index, 0)
    flip_x, flip_y, flip_z = flips((ROWS, LANES))
    stores = []
    for c, stage in exchange_plan(chunks, per_half):
        if stage < 0:
            loads[c].wait()
            operate(c)
            if c == 0:
                pl.semaphore_wait(barrier, 6)
            for l in range(per_half):
                start(c * per_half + l, 0)
            continue
        d = ORDERS[c % len(ORDERS)][stage]
        for copy in copies(c, stage):
            copy.wait()
        for side in range(2):
            e = side * (ctrl - 1)
            for f in range(2):
                if d == 0:
                    state[c, f, e] += xbuf[c, side, f]
                    continue
                for i in range(ctrl):
                    if d == 1:
                        state[c, f, i, e * ROWS : e * ROWS + ctrl] += ybuf[c, side, f, i]
                    else:
                        rows = pl.ds(e, ctrl, stride=ROWS)
                        state[c, f, i, rows, :] = state[c, f, i, rows, :] + zbuf[c, side, f, i]
        if stage < 2:
            start(c, stage + 1)
            continue
        lanes = slice(c * LANES, (c + 1) * LANES)
        for f in range(2):
            for i in range(ctrl):
                for j in range(ctrl):
                    x = [
                        [state[c, f, ii, jj * ROWS : (jj + 1) * ROWS] for jj in (j, ctrl - 1 - j)]
                        for ii in (i, ctrl - 1 - i)
                    ]
                    x = [jnp.where(flip_y, y[1], y[0]) for y in x]
                    x = jnp.where(flip_x, x[1], x[0])
                    other = jnp.take_along_axis(x, index, axis=0, mode="promise_in_bounds")
                    turned[f, i, j, :, lanes] = jnp.where(flip_z, other, x)[0:ctrl]
            store = pltpu.make_async_copy(
                turned.at[f, :, :, :, lanes],
                (stiff_hbm, mass_hbm)[f].at[:, :, :, lanes],
                out_sem.at[c, f],
            )
            store.start()
            stores.append(store)
    for store in stores:
        store.wait()


ORDERS = ((0, 2, 1), (1, 0, 2), (0, 2, 1), (1, 0, 2))
WIRE = (1.23, 2.15, 2.15)
LATENCY = (2.2, 2.2, 3.4)
COMPUTE = 1.7
FOLD = 0.3


def exchange_plan(chunks, per_part):
    free = [0.0, 0.0, 0.0]
    heap, plan = [], []

    def send(time, chunk, stage):
        d = ORDERS[chunk % len(ORDERS)][stage]
        free[d] = max(free[d], time) + WIRE[d]
        heapq.heappush(heap, (free[d] + LATENCY[d], chunk, stage))

    def arrivals(now, limit):
        while heap and heap[0][0] <= limit:
            time, chunk, stage = heapq.heappop(heap)
            now = max(now, time) + FOLD
            plan.append((chunk, stage))
            if stage < 2:
                send(now, chunk, stage + 1)
        return now

    now = 0.0
    for part in range(chunks // per_part):
        now = arrivals(now, now) + COMPUTE * per_part
        plan.append((part, -1))
        for chunk in range(part * per_part, (part + 1) * per_part):
            send(now, chunk, 0)
    arrivals(now, math.inf)
    return plan


def apply_patch(u, diag, off, weight, orient, values, slopes):
    quad, ctrl = values.shape
    vecs = u.shape[3]
    width = 2 * LANES
    halves = vecs // width
    chunks = vecs // LANES
    points = quad * quad
    size = ctrl * ROWS
    forward, backward = plane_tables(values, slopes)
    vmem = pl.BlockSpec(memory_space=pltpu.VMEM)
    hbm = pl.BlockSpec(memory_space=pl.ANY)
    f32 = jnp.float32
    return pl.pallas_call(
        functools.partial(patch_kernel, values, slopes),
        out_shape=[jax.ShapeDtypeStruct(u.shape, f32)] * 2,
        in_specs=[pl.BlockSpec(memory_space=pltpu.SMEM), hbm] + [vmem] * 5,
        out_specs=[hbm, hbm],
        scratch_shapes=[
            pltpu.VMEM((halves, ctrl, ctrl, ctrl, width), f32),
            pltpu.VMEM((2, ROWS, ROWS, width), f32),
            pltpu.VMEM((LANES, LANES), f32),
            pltpu.VMEM((7 * quad, points, LANES), f32),
            pltpu.VMEM((ctrl, 3 * points, width), f32),
            pltpu.VMEM((ctrl, 4 * points, width), f32),
            pltpu.VMEM((4 * size, 4 * points), jnp.bfloat16),
            pltpu.VMEM((chunks, 2, ctrl, size, LANES), f32),
            pltpu.VMEM((chunks, 2, 2, size, LANES), f32),
            pltpu.VMEM((chunks, 2, 2, ctrl, ctrl, LANES), f32),
            pltpu.VMEM((chunks, 2, 2, ctrl, ctrl, LANES), f32),
            pltpu.VMEM((chunks, 2, 2, ctrl, ctrl, LANES), f32),
            pltpu.VMEM((2, ctrl, ctrl, ctrl, vecs), f32),
            pltpu.SemaphoreType.DMA((halves,)),
            pltpu.SemaphoreType.DMA((chunks, 2)),
            pltpu.SemaphoreType.DMA((chunks, 3, 2)),
            pltpu.SemaphoreType.DMA((chunks, 3, 2)),
        ],
        compiler_params=pltpu.CompilerParams(collective_id=0, has_side_effects=True),
        name="apply_patch",
    )(orient, u, diag, off, weight, jnp.asarray(forward), jnp.asarray(backward))


def pass_kernel(stiff_in, mass_in, stiff_out, mass_out, buf, in_sem, out_sem):
    pieces = [(f, i) for i in range(buf.shape[1]) for f in range(2)]
    take = [
        pltpu.make_async_copy((stiff_in, mass_in)[f].at[i], buf.at[f, i], in_sem.at[f, i])
        for f, i in pieces
    ]
    give = [
        pltpu.make_async_copy(buf.at[f, i], (stiff_out, mass_out)[f].at[i], out_sem.at[f, i])
        for f, i in pieces
    ]
    for copy in take:
        copy.start()
    for first, second in zip(take, give):
        first.wait()
        second.start()
    for copy in give:
        copy.wait()


def pass_through(stiff, mass):
    hbm = pl.BlockSpec(memory_space=pl.ANY)
    return pl.pallas_call(
        pass_kernel,
        out_shape=[jax.ShapeDtypeStruct(stiff.shape, stiff.dtype)] * 2,
        in_specs=[hbm, hbm],
        out_specs=[hbm, hbm],
        scratch_shapes=[
            pltpu.VMEM((2,) + stiff.shape, stiff.dtype),
            pltpu.SemaphoreType.DMA((2, stiff.shape[0])),
            pltpu.SemaphoreType.DMA((2, stiff.shape[0])),
        ],
        name="pass_through",
    )(stiff, mass)


def per_device(control_values, metric_diag, metric_off, mass_weight, orient):
    values, slopes = spline_tables(mass_weight.shape[0] // 2)
    stiff, mass = apply_patch(
        control_values, metric_diag, metric_off, mass_weight, orient.reshape(3), values, slopes
    )
    return tuple(pass_through(stiff, mass))


def solution(mesh):
    in_specs = (
        P("px", "py", "pz", None),
        P(None, "px", ("py", "pz")),
        P(None, "px", ("py", "pz")),
        P("px", ("py", "pz")),
        P("px", "py", "pz", None),
    )
    out_specs = (P("px", "py", "pz", None), P("px", "py", "pz", None))
    return jax.shard_map(
        per_device, mesh=mesh, in_specs=in_specs, out_specs=out_specs, check_vma=False
    )
```
